32 devices in a mesh: rep: 2 (over x), exp: 2 (over core), tp: 8 (over z, y).
Axes of the slice: x: 2, y: 2, z: 4, core: 2. Of those that a mesh axis runs over, the one named last changes fastest.
Arguments:
- tokens: bfloat16 [1024, 4096], P(('rep', 'exp'), 'tp'), parts along dimension 0
- smooth_in: float32 [4096], P('tp'), may hold values from 0.5 to 2
- expert_ids: int32 [1024, 2], P(('rep', 'exp')), parts along dimension 0, may hold values from 0 to 3, as said below
- gate_fixed: int32 [1024, 2], P(('rep', 'exp')), parts along dimension 0, may hold values from 1 to 32767
- slots: int32 [1024, 2], P(('rep', 'exp')), parts along dimension 0, may hold values from 0 to 255, as said below
- w_gate: bfloat16 [4, 4096, 7168], P('exp', None, 'tp')
- w_up: bfloat16 [4, 4096, 7168], P('exp', None, 'tp')
- w_down: bfloat16 [4, 7168, 4096], P('exp', 'tp')
- gate_scale: float32 [4, 7168], P('exp', 'tp'), may hold values from 0.00010557433 to 0.0004222973
- up_scale: float32 [4, 7168], P('exp', 'tp'), may hold values from 0.00010557433 to 0.0004222973
- smooth_mid: float32 [4, 7168], P('exp', 'tp'), may hold values from 0.5 to 2
- down_scale: float32 [4, 4096], P('exp'), may hold values from 0.00015961338 to 0.0006384535
Outputs:
- moe_out: bfloat16 [1024, 4096], P(('rep', 'exp'), 'tp'), parts along dimension 0
The draws below stay inside these ranges and needn't reach their ends.
There are 2 independent parts, one for each index of `rep`. The reference program is written for one: setup_inputs(seed, part) draws one part's arguments, and reference() takes and returns one part's arrays. A program takes and returns all parts, laid end to end along the dimension named above; an argument that names none is the same for every part. Nothing has to cross between parts.
Inputs may be any that keep to these rules, and one draw needn't show every extreme that they name: `expert_ids`: the two experts of a token differ. Within one aligned block of 256 tokens (the tokens of one index of exp), the slots of the pairs that name one expert are distinct and run from 0 to their number less one. In every block some expert is named by 192 or more tokens.
All inputs are finite; a program needn't handle non-finite values.
Results may differ from the reference program's by a relative error of at most 0.006.
Values may be sent and summed in bfloat16 or wider, within the bound.
A program may use at most 128 MiB of HBM per device.

```python
import math
import jax
import jax.numpy as jnp
from jax import lax

D = 4096
FF = 7168
TOP = 2
BLK = 256
EXPERTS = 4
CAP = 192
TOKENS = 512


def routing(key):
    routing_key = jax.random.fold_in(key, 11)
    subkeys = jax.random.split(routing_key, 7)
    blocks = TOKENS // BLK
    hot_expert = jax.random.randint(subkeys[0], (), 0, EXPERTS)
    priority = jax.random.randint(subkeys[1], (blocks, BLK), 0, 1 << 20) * BLK + jnp.arange(BLK, dtype=jnp.int32)[None, :]
    position = jnp.argsort(jnp.argsort(priority, axis=1, stable=True), axis=1, stable=True)
    coin_flip = jax.random.randint(subkeys[2], (blocks, BLK), 0, 2)
    with_hot = ((position < CAP) | (coin_flip == 1)).reshape(TOKENS)
    first_off = jax.random.randint(subkeys[3], (TOKENS,), 1, EXPERTS)
    second_off = 1 + (first_off - 1 + jax.random.randint(subkeys[4], (TOKENS,), 1, EXPERTS - 1)) % (EXPERTS - 1)
    other_a = (hot_expert + first_off) % EXPERTS
    other_b = (hot_expert + second_off) % EXPERTS
    pair_one = jnp.where(with_hot, hot_expert, other_b)
    pair_two = other_a
    order_flip = jax.random.randint(subkeys[5], (TOKENS,), 0, 2)
    first = jnp.where(order_flip == 1, pair_two, pair_one)
    second = jnp.where(order_flip == 1, pair_one, pair_two)
    expert_list = jnp.stack([first, second], axis=1).astype(jnp.int32)
    slot_priority = jax.random.randint(subkeys[6], (blocks, 2 * BLK), 0, 1 << 20) * (2 * BLK) + jnp.arange(2 * BLK, dtype=jnp.int32)[None, :]
    flat_ids = expert_list.reshape(blocks, 2 * BLK)
    same_expert = flat_ids[:, :, None] == flat_ids[:, None, :]
    earlier = slot_priority[:, None, :] < slot_priority[:, :, None]
    slot_list = jnp.sum((same_expert & earlier).astype(jnp.int32), axis=2).reshape(TOKENS, 2)
    return (expert_list, slot_list.astype(jnp.int32))


def draw_expert_ids(key, part):
    expert_list, slot_list = routing(key)
    return expert_list


def draw_slots(key, part):
    expert_list, slot_list = routing(key)
    return slot_list


def int_weights(key, shape):
    return jax.random.randint(key, shape, -127, 128).astype(jnp.float32).astype(jnp.bfloat16)


def draw_w_gate(key, part):
    return int_weights(jax.random.fold_in(key, 1), (EXPERTS, D, FF))


def draw_w_up(key, part):
    return int_weights(jax.random.fold_in(key, 2), (EXPERTS, D, FF))


def draw_w_down(key, part):
    return int_weights(jax.random.fold_in(key, 3), (EXPERTS, FF, D))


def draw_tokens(key, part):
    subkeys = jax.random.split(jax.random.fold_in(key, 4), 3)
    column_scale = jnp.exp(jax.random.uniform(subkeys[0], (D,), jnp.float32, math.log(0.3), math.log(3.0)))
    row_scale = jnp.exp(jax.random.uniform(subkeys[1], (TOKENS, 1), jnp.float32, math.log(0.5), math.log(2.0)))
    values = jax.random.normal(subkeys[2], (TOKENS, D), jnp.float32)
    return (values * column_scale[None, :] * row_scale).astype(jnp.bfloat16)


def touch_ends(entries, own_key, smallest, high):
    longest = entries.shape.index(max(entries.shape))
    spots = []
    for shift in (0, 1):
        where = [jax.random.randint(jax.random.fold_in(own_key, axis), (), 0, length) for axis, length in enumerate(entries.shape)]
        where[longest] = (where[longest] + shift) % entries.shape[longest]
        spots.append(tuple(where))
    return entries.at[spots[0]].set(smallest).at[spots[1]].set(high)


def levels(rng, extent, cuts, least, top_value):
    def one(dim, blocks):
        draws = jax.random.uniform(jax.random.fold_in(jax.random.fold_in(rng, 6), dim), (blocks,), jnp.float32, least / len(cuts), top_value / len(cuts))
        return jnp.repeat(jnp.exp(draws), extent[dim] // blocks).reshape((-1,) + (1,) * (len(extent) - dim - 1))

    level = one(*cuts[0])
    for cut in cuts[1:]:
        level = level * one(*cut)
    return level


def setup_inputs(seed: int = 0, part: int = 0) -> dict:
    key_list = jax.random.split(jax.random.key(seed), 13)
    part_keys = jax.random.split(jax.random.fold_in(key_list[12], part), 13)
    return {
        "tokens": draw_tokens(jax.random.fold_in(jax.random.fold_in(key_list[12], part), 71), part),
        "smooth_in": jnp.clip(jnp.exp(math.log(2.0) - 1.3862944 * jax.random.uniform(key_list[1], (D,), jnp.float32) ** levels(key_list[1], (D,), ((0, 8),), -0.2, 0.2)), 0.5, 2.0),
        "expert_ids": draw_expert_ids(jax.random.fold_in(jax.random.fold_in(key_list[12], part), 71), part),
        "gate_fixed": touch_ends(jax.random.randint(part_keys[3], (TOKENS, TOP), 1, 32768), jax.random.fold_in(part_keys[3], 1), 1, 32767).astype(jnp.int32),
        "slots": draw_slots(jax.random.fold_in(jax.random.fold_in(key_list[12], part), 71), part),
        "w_gate": draw_w_gate(jax.random.fold_in(key_list[12], 71), part),
        "w_up": draw_w_up(jax.random.fold_in(key_list[12], 71), part),
        "w_down": draw_w_down(jax.random.fold_in(key_list[12], 71), part),
        "gate_scale": jnp.clip(jnp.exp(math.log(0.0004222973) - 1.3862944 * jax.random.uniform(key_list[8], (EXPERTS, FF), jnp.float32) ** levels(key_list[8], (EXPERTS, FF), ((0, 2), (1, 8)), -0.2, 0.2)), 0.00010557433, 0.0004222973),
        "up_scale": jnp.clip(jnp.exp(math.log(0.0004222973) - 1.3862944 * jax.random.uniform(key_list[9], (EXPERTS, FF), jnp.float32) ** levels(key_list[9], (EXPERTS, FF), ((0, 2), (1, 8)), -0.2, 0.2)), 0.00010557433, 0.0004222973),
        "smooth_mid": jnp.clip(jnp.exp(math.log(2.0) - 1.3862944 * jax.random.uniform(key_list[10], (EXPERTS, FF), jnp.float32) ** levels(key_list[10], (EXPERTS, FF), ((0, 2), (1, 8)), -0.2, 0.2)), 0.5, 2.0),
        "down_scale": jnp.clip(jnp.exp(math.log(0.0006384535) - 1.3862944 * jax.random.uniform(key_list[11], (EXPERTS, D), jnp.float32) ** levels(key_list[11], (EXPERTS, D), ((0, 2),), -0.2, 0.2)), 0.00015961338, 0.0006384535),
    }


CLIP_RATIO = 0.35
EPSILON = 1e-6


def expert_rows(quantized, in_scale, weights_of):
    gate_e, up_e, down_e, gate_sc, up_sc, smooth_e, down_sc = weights_of
    gate_pre = jnp.dot(quantized, gate_e, preferred_element_type=jnp.float32) * in_scale[:, None] * gate_sc[None, :]
    up_pre = jnp.dot(quantized, up_e, preferred_element_type=jnp.float32) * in_scale[:, None] * up_sc[None, :]
    hidden = jax.nn.silu(gate_pre) * up_pre / smooth_e[None, :]
    mid_scale = CLIP_RATIO * (jnp.max(jnp.abs(hidden), axis=1) + EPSILON) / 127.0
    hidden_q = jnp.clip(hidden / mid_scale[:, None], -127.0, 127.0).astype(jnp.bfloat16)
    down_acc = jnp.dot(hidden_q, down_e, preferred_element_type=jnp.float32)
    return down_acc * mid_scale[:, None] * down_sc[None, :]


def reference(tokens, smooth_in, expert_ids, gate_fixed, slots, w_gate, w_up, w_down, gate_scale, up_scale, smooth_mid, down_scale):
    smoothed = tokens.astype(jnp.float32) / smooth_in[None, :]
    in_scale = CLIP_RATIO * (jnp.max(jnp.abs(smoothed), axis=1) + EPSILON) / 127.0
    quantized = jnp.clip(smoothed / in_scale[:, None], -127.0, 127.0).astype(jnp.bfloat16)
    gate_values = gate_fixed.astype(jnp.float32)
    weight = gate_values / jnp.sum(gate_values, axis=1, keepdims=True)
    pair_weight = jnp.where(slots < CAP, weight, jnp.zeros_like(weight))

    def add_expert(accumulated, expert_index):
        weights_of = (w_gate[expert_index], w_up[expert_index], w_down[expert_index],
                      gate_scale[expert_index], up_scale[expert_index], smooth_mid[expert_index], down_scale[expert_index])
        produced = expert_rows(quantized, in_scale, weights_of)
        share = jnp.sum(jnp.where(expert_ids == expert_index, pair_weight, jnp.zeros_like(pair_weight)), axis=1)
        return accumulated + produced * share[:, None], expert_index

    start_sum = jnp.zeros((TOKENS, D), jnp.float32)
    accumulated, unused = lax.scan(add_expert, start_sum, jnp.arange(EXPERTS, dtype=jnp.int32))
    return accumulated.astype(jnp.bfloat16)
```

```python
import functools

import jax
import jax.numpy as jnp
from jax import lax
from jax.experimental import pallas as pl
from jax.experimental.pallas import tpu as pltpu
from jax.sharding import PartitionSpec as P

CLIP_RATIO = 0.35
EPSILON = 1e-06
LANES = 128
MESH = pl.DeviceIdType.MESH
F32 = jnp.float32
BF16 = jnp.bfloat16


def kernel(
    n, slots,
    tok_ref, smooth_ref, share_ref, wg_ref, wu_ref, wd_ref, gs_ref, us_ref, sm_ref, ds_ref,
    out_ref,
    x, wbuf, dbuf, acc, hq, meta, coef, pk, hx, hm, own, ssend, srecv, ysend, yrecv, comb, zsend, zrecv,
    w_sem, d_sem, pk_s, pk_r, hx_s, hx_r, meta_s, meta_r,
    az_s, ay_s, as_s, ag_r, as_r, rs_s, rs_r, ry_s, ry_r, rz_s, rz_r,
):
    q = n // 2
    me = lax.axis_index("tp")
    core = lax.axis_index("exp")
    z, y = me // 2, me % 2
    direction = 1 - 2 * (z % 2)
    experts = wg_ref.shape[0]
    block, depth = tok_ref.shape
    width = wg_ref.shape[2]

    def z_of(j):
        return (z + direction * j + q) % q

    def chunk(j, other):
        row = y + other * (1 - 2 * y)
        return z_of(j) * 2 + row

    def remote(src, dst, send, recv, device):
        return pltpu.make_async_remote_copy(
            src_ref=src, dst_ref=dst, send_sem=send, recv_sem=recv,
            device_id=device, device_id_type=MESH,
        )

    sibling = {"exp": 1 - core}
    partner = {"tp": chunk(0, 1)}

    def weight_copies(k):
        rows = pl.ds(pl.multiple_of(chunk(k // 2, k % 2) * depth, depth), depth)
        slot = k % slots
        return [
            pltpu.make_async_copy(ref.at[:, rows, :], wbuf.at[slot, i], w_sem.at[slot, i])
            for i, ref in enumerate((wg_ref, wu_ref))
        ]

    def down_copy(p):
        cols = pl.ds(pl.multiple_of(p * depth, depth), depth)
        return pltpu.make_async_copy(wd_ref.at[:, :, cols], dbuf.at[p], d_sem.at[p])

    for k in range(slots):
        for copy in weight_copies(k):
            copy.start()

    barrier = pltpu.get_barrier_semaphore()
    pl.semaphore_signal(barrier, inc=1, device_id=sibling, device_id_type=MESH)

    @pl.loop(1, n)
    def _(d):
        pl.semaphore_signal(barrier, inc=1, device_id={"tp": (me + d) % n}, device_id_type=MESH)

    smoothed = tok_ref[...].astype(F32) / smooth_ref[...]
    peak = jnp.max(jnp.abs(smoothed), axis=1, keepdims=True)
    peak_row = jnp.broadcast_to(peak, (block, LANES)).T[0:1, :]
    pk[pl.ds(me, 1)] = peak_row[None]

    pl.semaphore_wait(barrier, n)

    def pk_copy(d):
        return remote(pk.at[me], pk.at[me], pk_s.at[d], pk_r.at[me], {"tp": (me + d) % n})

    @pl.loop(1, n)
    def _(d):
        pk_copy(d).start()

    @pl.loop(0, 2 * experts)
    def _(t):
        acc[t] = jnp.zeros(acc.shape[1:], F32)

    @pl.loop(1, n)
    def _(d):
        p = (me + d) % n
        remote(pk.at[p], pk.at[p], pk_s.at[d], pk_r.at[p], {"tp": p}).wait_recv()

    row_peak = jnp.max(pk[0:n], axis=0)
    peak_col = jnp.broadcast_to(row_peak, (LANES, block)).T
    in_scale = CLIP_RATIO * (peak_col + EPSILON) / 127.0
    smoothed = tok_ref[...].astype(F32) / smooth_ref[...]
    x[me, core] = jnp.clip(smoothed / in_scale[:, 0:1], -127.0, 127.0).astype(BF16)
    lane = lax.broadcasted_iota(jnp.int32, (block, LANES), 1)
    meta[core] = jnp.where(lane < 2 * experts, share_ref[...], in_scale)

    def z_copy(j):
        return remote(x.at[me, core], x.at[me, core], az_s.at[j], ag_r.at[me], {"tp": chunk(j, 0)})

    def y_copy(j):
        p = chunk(j, 0)
        return remote(x.at[p, core], x.at[p, core], ay_s.at[j], ag_r.at[p], partner)

    def sib_copy(p, b):
        return remote(x.at[p, b], x.at[p, b], as_s.at[p], as_r.at[p], sibling)

    def arrived(p):
        remote(x.at[p, core], x.at[p, core], as_s.at[p], ag_r.at[p], sibling).wait_recv()

    y_copy(0).start()

    @pl.loop(1, q)
    def _(j):
        z_copy(j).start()

    meta_copy = remote(meta.at[core], meta.at[core], meta_s, meta_r, sibling)
    meta_copy.start()
    sib_copy(me, core).start()

    def compute(k):
        p = chunk(k // 2, k % 2)
        slot = k % slots
        for copy in weight_copies(k):
            copy.wait()
        sib_copy(p, 1 - core).wait_recv()

        @pl.loop(0, 2 * experts)
        def _(t):
            acc[t] += jnp.dot(
                x[p].reshape(2 * block, depth), wbuf[slot, t // experts, t % experts],
                preferred_element_type=F32,
            )

        @pl.when(k + slots < n)
        def _():
            for copy in weight_copies(k + slots):
                copy.start()

        down_copy(p).start()

    compute(0)
    arrived(chunk(0, 1))
    sib_copy(chunk(0, 1), core).start()

    @pl.loop(1, q)
    def _(j):
        p = chunk(j, 0)
        arrived(p)
        y_copy(j).start()
        sib_copy(p, core).start()
        compute(2 * j - 1)
        compute(2 * j)
        p = chunk(j, 1)
        arrived(p)
        sib_copy(p, core).start()

    compute(n - 1)
    meta_copy.wait_recv()

    rb = 32
    blocks = block // rb
    for e in range(experts):

        @pl.loop(0, 2 * blocks)
        def _(r):
            rows = pl.ds(pl.multiple_of(r * rb, rb), rb)
            inner = pl.ds(pl.multiple_of((r % blocks) * rb, rb), rb)
            scale = meta[r // blocks, inner, :][:, LANES - 1:]
            gate = acc[e, rows, :] * scale * gs_ref[...][e:e + 1]
            up = acc[experts + e, rows, :] * scale * us_ref[...][e:e + 1]
            hidden = gate / (1.0 + jnp.exp(-gate)) * up / sm_ref[...][e:e + 1]
            acc[e, rows, :] = hidden
            hm[rows, :] = jnp.broadcast_to(jnp.max(jnp.abs(hidden), axis=1, keepdims=True), (rb, LANES))

        hx[pl.ds(me, 1), e:e + 1, :] = hm[...].T[0:1, :][None]

    def hx_copy(d):
        return remote(hx.at[me], hx.at[me], hx_s.at[d], hx_r.at[me], {"tp": (me + d) % n})

    @pl.loop(1, n)
    def _(d):
        hx_copy(d).start()

    @pl.loop(1, n)
    def _(d):
        p = (me + d) % n
        remote(hx.at[p], hx.at[p], hx_s.at[d], hx_r.at[p], {"tp": p}).wait_recv()

    mid_rows = CLIP_RATIO * (jnp.max(hx[0:n], axis=0) + EPSILON) / 127.0
    for e in range(experts):
        coef[e] = jnp.broadcast_to(mid_rows[e:e + 1, :], (LANES, 2 * block)).T

        @pl.loop(0, 2 * blocks)
        def _(r):
            rows = pl.ds(pl.multiple_of(r * rb, rb), rb)
            inner = pl.ds(pl.multiple_of((r % blocks) * rb, rb), rb)
            mid = coef[e, rows, :]
            hq[e, rows, :] = jnp.clip(acc[e, rows, :] * (1.0 / mid[:, 0:1]), -127.0, 127.0).astype(BF16)
            lanes = lax.broadcasted_iota(jnp.int32, (rb, LANES), 1)
            picked = jnp.where(lanes == core * experts + e, meta[r // blocks, inner, :], 0.0)
            coef[e, rows, :] = mid * jnp.sum(picked, axis=1, keepdims=True)

    def partial(p, b):
        rows = pl.ds(pl.multiple_of(b * block, block), block)
        cols = pl.ds(pl.multiple_of(p * depth, depth), depth)
        total = None
        for e in range(experts):
            part = jnp.dot(hq[e, rows, :], dbuf[p, e], preferred_element_type=F32)
            part = part * coef[e, rows, 0:1] * ds_ref[:, cols][e:e + 1]
            total = part if total is None else total + part
        return total

    def shard_of(k):
        return chunk(q - 1 - k % q, 1 - k // q)

    def rs_copy(k):
        return remote(ssend.at[k], srecv.at[k], rs_s.at[k], rs_r.at[k], sibling)

    def ry_copy(j):
        return remote(ysend.at[j], yrecv.at[j], ry_s.at[j], ry_r.at[j], partner)

    def rz_copy(j):
        return remote(zsend.at[j], zrecv.at[z], rz_s.at[j], rz_r.at[z], {"tp": chunk(j, 0)})

    def combine(k):
        j = q - 1 - k % q
        rs_copy(k).wait_recv()

        @pl.when(k < q)
        def _():
            ysend[j] = (own[k % 2] + srecv[k].astype(F32)).astype(BF16)
            ry_copy(j).start()

        @pl.when(k >= q)
        def _():
            comb[j] = own[k % 2] + srecv[k].astype(F32)

    @pl.loop(0, n)
    def _(k):
        p = shard_of(k)
        down_copy(p).wait()
        ssend[k] = partial(p, 1 - core).astype(BF16)
        rs_copy(k).start()
        own[k % 2] = partial(p, core)

        @pl.when(k > 0)
        def _():
            combine(k - 1)

    combine(n - 1)

    @pl.loop(0, q - 1)
    def _(i):
        j = q - 1 - i
        ry_copy(j).wait_recv()
        zsend[j] = (comb[j] + yrecv[j].astype(F32)).astype(BF16)
        rz_copy(j).start()

    ry_copy(0).wait_recv()
    comb[0] += yrecv[0].astype(F32)

    @pl.loop(1, q)
    def _(j):
        s = z_of(j)
        remote(zsend.at[j], zrecv.at[s], rz_s.at[j], rz_r.at[s], sibling).wait_recv()
        comb[0] += zrecv[s].astype(F32)

    out_ref[...] = comb[0].astype(BF16)

    meta_copy.wait_send()

    @pl.loop(1, n)
    def _(d):
        pk_copy(d).wait_send()
        hx_copy(d).wait_send()

    @pl.loop(0, n)
    def _(k):
        sib_copy(k, core).wait_send()
        rs_copy(k).wait_send()

    @pl.loop(0, q)
    def _(j):
        y_copy(j).wait_send()
        ry_copy(j).wait_send()

    @pl.loop(1, q)
    def _(j):
        z_copy(j).wait_send()
        rz_copy(j).wait_send()


def per_device(
    n,
    tokens, smooth_in, expert_ids, gate_fixed, slots,
    w_gate, w_up, w_down, gate_scale, up_scale, smooth_mid, down_scale,
):
    q = n // 2
    experts, _, width = w_gate.shape
    block, depth = tokens.shape
    capacity = 3 * block // 4
    gate_values = gate_fixed.astype(F32)
    weight = gate_values / jnp.sum(gate_values, axis=1, keepdims=True)
    pair_weight = jnp.where(slots < capacity, weight, 0.0)
    lane = jnp.arange(LANES, dtype=jnp.int32)[None, :]
    share = sum(
        jnp.where(expert_ids[:, k:k + 1] == lane, pair_weight[:, k:k + 1], 0.0)
        for k in range(expert_ids.shape[1])
    )
    ring = min(n, 5)
    vmem = pl.BlockSpec(memory_space=pltpu.VMEM)
    hbm = pl.BlockSpec(memory_space=pl.ANY)
    dma = pltpu.SemaphoreType.DMA
    slab = (block, depth)
    return pl.pallas_call(
        functools.partial(kernel, n, ring),
        out_shape=jax.ShapeDtypeStruct(slab, BF16),
        in_specs=[vmem] * 3 + [hbm] * 3 + [vmem] * 4,
        out_specs=vmem,
        scratch_shapes=[
            pltpu.VMEM((n, 2, *slab), BF16),
            pltpu.VMEM((ring, 2, experts, depth, width), BF16),
            pltpu.VMEM((n, experts, width, depth), BF16),
            pltpu.VMEM((2 * experts, 2 * block, width), F32),
            pltpu.VMEM((experts, 2 * block, width), BF16),
            pltpu.VMEM((2, block, LANES), F32),
            pltpu.VMEM((experts, 2 * block, LANES), F32),
            pltpu.VMEM((n + 8, 1, block), F32),
            pltpu.VMEM((n + 8, experts, 2 * block), F32),
            pltpu.VMEM((2 * block, LANES), F32),
            pltpu.VMEM((2, *slab), F32),
            pltpu.VMEM((n, *slab), BF16),
            pltpu.VMEM((n, *slab), BF16),
            pltpu.VMEM((q, *slab), BF16),
            pltpu.VMEM((q, *slab), BF16),
            pltpu.VMEM((q, *slab), F32),
            pltpu.VMEM((q, *slab), BF16),
            pltpu.VMEM((q, *slab), BF16),
            dma((ring, 2)), dma((n,)), dma((n,)), dma((n,)), dma((n,)), dma((n,)), dma, dma,
            dma((q,)), dma((q,)), dma((n,)), dma((n,)), dma((n,)),
            dma((n,)), dma((n,)), dma((q,)), dma((q,)), dma((q,)), dma((q,)),
        ],
        compiler_params=pltpu.CompilerParams(
            collective_id=0, has_side_effects=True, vmem_limit_bytes=67043328
        ),
    )(tokens, smooth_in[None, :], share, w_gate, w_up, w_down, gate_scale, up_scale, smooth_mid, down_scale)


def solution(mesh):
    n = mesh.shape["tp"]
    in_specs = (
        P(("rep", "exp"), "tp"),
        P("tp"),
        P(("rep", "exp"), None),
        P(("rep", "exp"), None),
        P(("rep", "exp"), None),
        P("exp", None, "tp"),
        P("exp", None, "tp"),
        P("exp", "tp", None),
        P("exp", "tp"),
        P("exp", "tp"),
        P("exp", "tp"),
        P("exp", None),
    )
    out_specs = P(("rep", "exp"), "tp")
    return jax.shard_map(
        functools.partial(per_device, n), mesh=mesh, in_specs=in_specs, out_specs=out_specs, check_vma=False
    )
```
